32 devices in a mesh: adapter: 16 (over z, y, x), mp: 2 (over core).
Axes of the slice: x: 2, y: 2, z: 4, core: 2. Of those that a mesh axis runs over, the one named last changes fastest.
Arguments:
- hidden: bfloat16 [4096, 4096], P('adapter', 'mp'), may hold values from -8 to 8
- subsets: int32 [4096, 8], P('adapter'), may hold values from 0 to 15, all different within a row; in each aligned block of 256 rows (0 to 255, 256 to 511, ...) at most 256 rows name the same one
- down_weight: bfloat16 [16, 4096, 256], P('adapter', 'mp'), may hold values from -0.09375 to 0.09375
- up_weight: bfloat16 [16, 256, 4096], P('adapter', None, 'mp'), may hold values from -0.375 to 0.375
- query_weight: bfloat16 [4096, 4096], P('mp'), may hold values from -0.08 to 2.08
- key_weight: bfloat16 [4096, 4096], P('mp'), may hold values from -0.08 to 2.08
Outputs:
- joined: bfloat16 [4096, 4096], P('adapter', 'mp')
The draws below stay inside these ranges and needn't reach their ends.
Inputs may be any that keep to these rules, and one draw needn't show every extreme that they name: `subsets`: each row names 8 different adapters; within the rows of one index of the adapter axis no adapter is named by more than 256 rows.
All inputs are finite; a program needn't handle non-finite values.
Results may differ from the reference program's by a relative error of at most 0.025.
Values may be sent and summed in bfloat16 or wider, within the bound.
A program may use at most 192 MiB of HBM per device.

```python
import math
import jax
import jax.numpy as jnp
import numpy as np
from jax import lax

D = 4096
B = 256
K = 8
REQ_DEV = 256
ADAPTERS = 16
REQUESTS = 4096
CAP = 256


def draw_hidden(key, part):
    values = jnp.clip(jax.random.normal(key, (REQUESTS, D), jnp.float32), -5.0, 5.0)
    return values.astype(jnp.bfloat16)


def draw_query_weight(key, part):
    values = jnp.clip(jax.random.normal(jax.random.fold_in(key, 11), (D, D), jnp.float32) * D ** (-0.5), -0.078125, 0.078125)
    return values.astype(jnp.bfloat16)


def draw_key_weight(key, part):
    values = jnp.clip(jax.random.normal(jax.random.fold_in(key, 13), (D, D), jnp.float32) * D ** (-0.5), -0.078125, 0.078125)
    return values.astype(jnp.bfloat16)


def level_of(rng, extent, pieces, least, high):
    gain = 1.0
    for axis_at, parts in pieces:
        draws = jax.random.uniform(jax.random.fold_in(jax.random.fold_in(rng, 6), axis_at), (parts,), jnp.float32, least / len(pieces), high / len(pieces))
        gain = gain * jnp.repeat(jnp.exp(draws), extent[axis_at] // parts).reshape((-1,) + (1,) * (len(extent) - 1 - axis_at))
    return gain


def shared_out(stream_key, own, number, rows, count, top, reach, lean):
    ranking = jax.random.permutation(stream_key, count)
    crowded, common = shares(count, rows * top, reach, lean, True), shares(count, rows * top, reach, lean, False)
    places = jnp.arange(count)

    def named(tallies, offset_by):
        used = int((tallies > 0).sum())
        fixed = max(1, used // 4)
        moved = fixed + (places - fixed + offset_by * (used - fixed)) % max(1, count - fixed)
        return jnp.zeros((count,), jnp.int32).at[ranking[jnp.where(places < fixed, places, moved)]].set(jnp.asarray(tallies, jnp.int32))

    tallies = jnp.where(number % 4 == 0, named(crowded, number // 4), named(common, number - number // 4 - 1))
    mixed = jax.random.permutation(jax.random.fold_in(own, 3), count)
    source_of, receiver = mixed[0:count // 2 * 2:2], mixed[1:count // 2 * 2:2]
    slack = jnp.minimum(tallies[source_of] - 1, reach - tallies[receiver]) // 2
    slack = jnp.where((source_of == ranking[0]) | (receiver == ranking[0]) | (tallies[receiver] == 0), 0, jnp.maximum(slack, 0))
    moved = jax.random.randint(jax.random.fold_in(own, 4), (count // 2,), 0, 1 << 20) % (slack + 1)
    tallies = tallies.at[source_of].add(-moved).at[receiver].add(moved)
    items = jnp.searchsorted(jnp.cumsum(tallies), jnp.arange(rows * top), side="right").astype(jnp.int32)
    table = items.reshape(top, rows).T
    table = table[jax.random.permutation(jax.random.fold_in(own, 1), rows)]
    offset_by = jax.random.randint(jax.random.fold_in(own, 2), (rows, 1), 0, top)
    return jnp.take_along_axis(table, (jnp.arange(top)[None, :] + offset_by) % top, axis=1)


def shares(number_of, total, bound, slope, full):
    weights = [(1 << 20) // math.isqrt(rank ** slope) + 1 for rank in range(1, number_of + 1)]
    largest = bound if full else min(bound, max(-(-total // number_of), total * weights[0] // sum(weights)))
    least = 1 if total - largest >= number_of - 1 else 0
    counts, surplus = [largest] + [least] * (number_of - 1), total - largest - least * (number_of - 1)
    while surplus > 0:
        candidates = [i for i in range(1, number_of) if counts[i] < largest] or [i for i in range(1, number_of) if counts[i] < bound]
        mass, left = sum([weights[i] for i in candidates]), surplus
        for i in candidates:
            extra = min(bound - counts[i], max(1, left * weights[i] // mass), surplus)
            counts[i] = counts[i] + extra
            surplus = surplus - extra
    return np.array(counts)


def bell_draw(rng, extent, spread, limit, pieces=(), kind=jnp.bfloat16):
    result = spread * jax.random.normal(rng, extent, jnp.float32)
    if pieces:
        result = result * level_of(rng, extent, pieces, -0.22, 0.18)
    return jnp.clip(result, -limit, limit).astype(kind)


def setup_inputs(seed: int = 0) -> dict:
    seeds = jax.random.split(jax.random.key(seed), 7)
    hidden = draw_hidden(jax.random.fold_in(seeds[6], 71), 0)
    subsets_keys = jax.random.split(jax.random.fold_in(seeds[1], 1), REQUESTS // REQ_DEV)
    subsets_turns = jax.random.permutation(jax.random.fold_in(seeds[1], 3), REQUESTS // REQ_DEV)
    subsets = jax.vmap(lambda own, number: shared_out(jax.random.fold_in(seeds[1], 2), own, number, REQ_DEV, ADAPTERS, K, CAP, 2))(subsets_keys, subsets_turns).reshape((REQUESTS, K))
    down_weight = bell_draw(seeds[2], (ADAPTERS, D, B), D ** -0.5, 0.09375, ((0, 16), (1, 2)))
    up_weight = bell_draw(seeds[3], (ADAPTERS, B, D), B ** -0.5, 0.375, ((0, 16), (2, 2)))
    query_weight = draw_query_weight(jax.random.fold_in(seeds[6], 71), 0)
    key_weight = draw_key_weight(jax.random.fold_in(seeds[6], 71), 0)
    return dict(hidden=hidden, subsets=subsets, down_weight=down_weight, up_weight=up_weight, query_weight=query_weight, key_weight=key_weight)


def reference(hidden, subsets, down_weight, up_weight, query_weight, key_weight):
    query = jnp.dot(hidden, query_weight, preferred_element_type=jnp.float32).astype(jnp.bfloat16)
    probe = lax.dot_general(query, key_weight, (((1,), (1,)), ((), ())), preferred_element_type=jnp.float32).astype(jnp.bfloat16)

    def visit(gathered, operands):
        index, down_one, up_one = operands
        bottle = jnp.maximum(jnp.dot(hidden, down_one, preferred_element_type=jnp.float32), 0.0).astype(jnp.bfloat16)
        produced = jnp.dot(bottle, up_one, preferred_element_type=jnp.float32).astype(jnp.bfloat16)
        landed = subsets == index
        gathered = jnp.where(landed[:, :, None], produced[:, None, :], gathered)
        return gathered, None

    start_value = jnp.zeros((REQUESTS, K, D), jnp.bfloat16)
    picked, _ = lax.scan(visit, start_value, (jnp.arange(ADAPTERS, dtype=jnp.int32), down_weight, up_weight))
    widened = picked.astype(jnp.float32)
    base = hidden.astype(jnp.float32)
    probe_wide = probe.astype(jnp.float32)
    own_term = jnp.sum(base * probe_wide, axis=1)
    logits = (jnp.einsum("rkd,rd->rk", widened, probe_wide, precision=lax.Precision.HIGHEST) + own_term[:, None]) * (D ** -0.5)
    share = jax.nn.softmax(logits, axis=-1)
    joined = base + jnp.einsum("rk,rkd->rd", share, widened, precision=lax.Precision.HIGHEST)
    return joined.astype(jnp.bfloat16)
```

```python
import functools

import jax
import jax.numpy as jnp
import numpy as np
from jax import lax
from jax.experimental import pallas as pl
from jax.experimental.pallas import tpu as pltpu
from jax.sharding import PartitionSpec as P


f32, bf16 = jnp.float32, jnp.bfloat16


def both_cores(part):
    size = lax.axis_size("mp")
    total = part
    for shift in range(1, size):
        total = total + lax.ppermute(part, "mp", [(i, (i + shift) % size) for i in range(size)])
    return total


MESH = pl.DeviceIdType.MESH
NEVER = -1e30
VMEM_BYTES = 67_000_000
QUERY_TILE, KEY_TILE, DEPTH = 512, 256, 3
DOWN_PARTS, UP_PARTS = 2, 4
NT = (((1,), (1,)), ((), ()))


def dot(a, b):
    return jnp.dot(a, b, preferred_element_type=f32)


def dot_nt(a, b):
    return lax.dot_general(a, b, NT, preferred_element_type=f32)


def kernel(
    bits, hid_in, sub_in, down_in, up_in, query_in, key_in, out,
    hid, sub, down, up, query, query_got, probe, wide, wide_got, level, turned,
    mine, mine_got, masked, theirs, sent, got, total, query_tile, key_tile,
    send, recv, query_send, query_recv, local, query_sem, key_sem,
):
    east, above, side, across = bits
    rows, width = hid_in.shape
    model = query_in.shape[1]
    depth = down_in.shape[1]
    everyone = 4 * rows
    me, core = lax.axis_index("adapter"), lax.axis_index("mp")

    def flip(index, bit):
        return index + bit * (1 - 2 * ((index // bit) % 2))

    to_east, to_above = (flip(me, east), core), (flip(me, above), core)
    to_corner = (flip(flip(me, east), above), core)
    to_side, to_across, to_core = (flip(me, side), core), (flip(me, across), core), (me, 1 - core)

    count = [0]

    def remote(src, dst, where):
        i = count[0]
        count[0] += 1
        return pltpu.make_async_remote_copy(
            src_ref=src, dst_ref=dst, send_sem=send.at[i], recv_sem=recv.at[i],
            device_id=where, device_id_type=MESH,
        )

    def block(ref, b, start=0, size=rows):
        return ref.at[pl.ds(b * rows + start, size), :]

    half = rows // 2
    hid_above = [remote(hid_in.at[pl.ds(h * half, half), :], block(hid, 2, h * half, half), to_above) for h in (0, 1)]
    hid_east = [remote(hid_in.at[pl.ds(h * half, half), :], block(hid, 1, h * half, half), to_east) for h in (0, 1)]
    hid_corner = [
        remote(block(hid, 2, 0, half), block(hid, 3, 0, half), to_east),
        remote(block(hid, 1, half, half), block(hid, 3, half, half), to_above),
    ]
    subs = [remote(sub_in, sub.at[k], w) for k, w in ((1, to_east), (2, to_above), (3, to_corner))]

    def down_cut(ref, c):
        size = width // DOWN_PARTS
        return ref.at[pl.ds(c * size, size), :]

    def up_cut(ref, m, c):
        size = width // UP_PARTS
        return ref.at[pl.ds(m * depth, depth), pl.ds(c * size, size)]

    down_side = remote(down_in, down.at[1], to_side)
    up_side = remote(up_in, up.at[pl.ds(depth, depth), :], to_side)
    down_across = [remote(down_cut(down_in, c), down_cut(down.at[2], c), to_across) for c in range(DOWN_PARTS)]
    up_across = [remote(up_cut(up_in, 0, c), up_cut(up, 2, c), to_across) for c in range(UP_PARTS)]
    down_relay = [remote(down_cut(down.at[2], c), down_cut(down.at[3], c), to_side) for c in range(DOWN_PARTS)]
    up_relay = [remote(up_cut(up, 2, c), up_cut(up, 3, c), to_side) for c in range(UP_PARTS)]
    wides = [
        remote(wide.at[:, pl.ds(m * depth, depth)], wide_got.at[:, pl.ds(m * depth, depth)], to_core)
        for m in range(4)
    ]
    mines = remote(mine, mine_got, to_core)
    tells = [remote(masked, theirs.at[k - 1], w) for k, w in ((1, to_east), (2, to_above), (3, to_corner))]
    piece = width // 4
    hops = [(to_east, to_above), (to_above, to_east)]
    outs = {
        (kind, h, q): remote(sent.at[kind, 2 * h + q], got.at[kind, 2 * h + q], hops[h][0 if kind < 2 else 1])
        for kind in range(3) for h in range(2) for q in range(2)
    }

    own_hid = pltpu.make_async_copy(hid_in, block(hid, 0), local.at[0])
    own_down = pltpu.make_async_copy(down_in, down.at[0], local.at[1])
    own_up = pltpu.make_async_copy(up_in, up.at[pl.ds(0, depth), :], local.at[2])
    own_sub = pltpu.make_async_copy(sub_in, sub.at[0], local.at[3])

    query_tiles, key_tiles = model // QUERY_TILE, width // KEY_TILE

    def query_fetch(j):
        s = lax.rem(j, DEPTH)
        return pltpu.make_async_copy(
            query_in.at[:, pl.ds(j * QUERY_TILE, QUERY_TILE)], query_tile.at[s], query_sem.at[s])

    def key_fetch(j):
        s = lax.rem(j, DEPTH)
        return pltpu.make_async_copy(
            key_in.at[pl.ds(j * KEY_TILE, KEY_TILE), :], key_tile.at[s], key_sem.at[s])

    def ahead(fetch):
        for j in range(DEPTH - 1):
            fetch(jnp.int32(j)).start()

    def follow(fetch, j, tiles):
        @pl.when(j + (DEPTH - 1) < tiles)
        def _():
            fetch(j + (DEPTH - 1)).start()

        fetch(j).wait()

    def query_send_tile(turn, start, size, j):
        at = (pl.ds(start, size), pl.ds(j * QUERY_TILE, QUERY_TILE))
        i = turn * query_tiles + j
        return pltpu.make_async_remote_copy(
            src_ref=query.at[at], dst_ref=query_got.at[at], send_sem=query_send.at[i], recv_sem=query_recv.at[i],
            device_id=to_core, device_id_type=MESH,
        )

    def query_part(turn, start, size):
        def step(j, _):
            follow(query_fetch, j, query_tiles)
            tile = dot(hid[pl.ds(start, size), :], query_tile[lax.rem(j, DEPTH)])
            query[pl.ds(start, size), pl.ds(pl.multiple_of(j * QUERY_TILE, QUERY_TILE), QUERY_TILE)] = tile.astype(bf16)

            @pl.when(j > 0)
            def _():
                query_send_tile(turn, start, size, j - 1).start()

            return 0

        lax.fori_loop(0, query_tiles, step, 0)

    def query_sum(turn, start, size):
        def step(j, _):
            query_send_tile(turn, start, size, j).wait()
            at = (pl.ds(start, size), pl.ds(pl.multiple_of(j * QUERY_TILE, QUERY_TILE), QUERY_TILE))
            query[at] = query[at] + query_got[at]
            return 0

        lax.fori_loop(0, query_tiles, step, 0)

    def probe_part(start, size, low, high):
        def step(j, _):
            follow(key_fetch, j, key_tiles)
            tile = dot_nt(query[pl.ds(start, size), :], key_tile[lax.rem(j, DEPTH)])
            probe[pl.ds(start, size), pl.ds(pl.multiple_of(j * KEY_TILE, KEY_TILE), KEY_TILE)] = tile.astype(bf16)
            return 0

        lax.fori_loop(low, high, step, 0)

    def bottle(m):
        def step(c, _):
            at = pl.ds(pl.multiple_of(c * rows, rows), rows)
            wide[at, pl.ds(m * depth, depth)] = dot(hid[at, :], down[m]).astype(bf16)
            return 0

        lax.fori_loop(0, 4, step, 0)

    def own_term():
        def step(c, _):
            at = pl.ds(pl.multiple_of(c * rows // 4, rows // 4), rows // 4)
            term = jnp.sum(hid[at, :].astype(f32) * probe[at, :].astype(f32), axis=1, keepdims=True)
            level[at, :] = jnp.broadcast_to(term, (rows // 4, level.shape[1]))
            return 0

        lax.fori_loop(0, 16, step, 0)

    def reach(m):
        columns = pl.ds(m * depth, depth)

        def step(c, _):
            at = pl.ds(pl.multiple_of(c * rows, rows), rows)
            there = dot_nt(probe[at, :], up[columns, :])
            kept = jnp.maximum(wide[at, columns] + wide_got[at, columns], 0)
            wide[at, columns] = kept
            term = jnp.sum(kept.astype(f32) * there, axis=1, keepdims=True)
            lane = lax.broadcasted_iota(jnp.int32, (rows, level.shape[1]), 1)
            level[at, :] = level[at, :] + jnp.where(lane == m, term, 0.0)
            return 0

        lax.fori_loop(0, 4, step, 0)

    barrier = pltpu.get_barrier_semaphore()
    partners = (to_east, to_above, to_corner, to_side, to_across, to_core)
    for where in partners:
        pl.semaphore_signal(barrier, inc=1, device_id=where, device_id_type=MESH)
    pl.semaphore_wait(barrier, len(partners))

    hid_above[0].start()
    hid_east[1].start()
    own_hid.start()
    ahead(query_fetch)
    hid_above[1].start()
    hid_east[0].start()
    for copy in subs + down_across + [down_side, up_side, own_down, own_up, own_sub]:
        copy.start()
    ahead(key_fetch)

    own_hid.wait()
    query_part(0, 0, rows)
    query_send_tile(0, 0, rows, query_tiles - 1).start()
    ahead(query_fetch)
    query_sum(0, 0, rows)
    probe_part(0, rows, 0, key_tiles)
    ahead(key_fetch)

    hid_above[0].wait_recv()
    hid_corner[0].start()
    hid_east[1].wait_recv()
    hid_corner[1].start()
    for copy in up_across:
        copy.start()
    hid_above[1].wait_recv()
    hid_east[0].wait_recv()
    own_down.wait()
    hid_corner[0].wait_recv()
    hid_corner[1].wait_recv()
    bottle(0)
    down_side.wait_recv()
    bottle(1)
    wides[0].start()
    query_part(1, rows, 3 * rows)
    wides[1].start()
    query_send_tile(1, rows, 3 * rows, query_tiles - 1).start()
    for c in range(DOWN_PARTS):
        down_across[c].wait_recv()
        down_relay[c].start()
    bottle(2)
    query_sum(1, rows, 3 * rows)
    wides[2].start()
    probe_part(rows, 3 * rows, 0, key_tiles // 2)
    up_across[0].wait_recv()
    up_relay[0].start()
    probe_part(rows, 3 * rows, key_tiles // 2, key_tiles)
    up_across[1].wait_recv()
    up_relay[1].start()
    own_term()
    own_up.wait()
    wides[0].wait()
    reach(0)
    up_across[2].wait_recv()
    up_relay[2].start()
    up_side.wait_recv()
    wides[1].wait()
    reach(1)
    for c in range(DOWN_PARTS):
        down_relay[c].wait_recv()
    bottle(3)
    up_across[3].wait_recv()
    up_relay[3].start()
    wides[3].start()
    wides[2].wait()
    reach(2)
    wides[3].wait()
    for c in range(UP_PARTS):
        up_relay[c].wait_recv()
    reach(3)

    mine[...] = jnp.transpose(level[...])[:8]
    for copy in subs:
        copy.wait_recv()
    own_sub.wait()
    turned[...] = jnp.zeros_like(turned)
    line = lax.broadcasted_iota(jnp.int32, (8, rows), 0)
    labels = [me, flip(me, side), flip(me, across), flip(flip(me, side), across)]
    named = []
    for b in range(4):
        marks = jnp.zeros((8, rows), f32)
        for m in range(4):
            hit = jnp.max((sub[b] == labels[m]).astype(f32), axis=0, keepdims=True)
            marks = jnp.where(line == m, hit, marks)
        named.append(marks)
    mines.start()
    mines.wait()
    for b in range(4):
        at = pl.ds(b * rows, rows)
        logit = (mine[:, at] + mine_got[:, at]) * model ** (-0.5)
        masked[:, at] = jnp.where(named[b] > 0, logit, NEVER)
    for copy in tells:
        copy.start()
    for copy in tells:
        copy.wait()
    for b in range(4):
        at = pl.ds(b * rows, rows)
        own = masked[:, at]
        others = [theirs[k - 1][:, (b ^ k) * rows : ((b ^ k) + 1) * rows] for k in (1, 2, 3)]
        peak = own
        for other in others:
            peak = jnp.maximum(peak, other)
        peak = jnp.max(peak, axis=0, keepdims=True)
        mass = jnp.exp(own - peak)
        whole = mass
        for other in others:
            whole = whole + jnp.exp(other - peak)
        turned[0:8, at] = mass / jnp.sum(whole, axis=0, keepdims=True)
    level[...] = jnp.transpose(turned[...])

    def weigh(b):
        at = pl.ds(b * rows, rows)
        for m in range(4):
            columns = pl.ds(m * depth, depth)
            wide[at, columns] = (wide[at, columns].astype(f32) * level[at, m : m + 1]).astype(bf16)

    def product(b, h, q):
        return dot(wide[pl.ds(b * rows, rows), :], up[:, pl.ds((2 * h + q) * piece, piece)])

    pending = []

    def post(copy):
        if pending:
            pending.pop().start()
        if copy is not None:
            pending.append(copy)

    order = [(h, q) for q in range(2) for h in range(2)]
    weigh(3)
    for h, q in order:
        sent[0, 2 * h + q] = product(3, h, q).astype(bf16)
        post(outs[0, h, q])
    weigh(1)
    weigh(2)
    for h, q in order:
        sent[1, 2 * h + q] = product((1, 2)[h], h, q).astype(bf16)
        post(outs[1, h, q])
    weigh(0)
    for h, q in order:
        at = pl.ds((2 * h + q) * piece, piece)
        total[:, at] = hid[pl.ds(0, rows), at].astype(f32) + product(0, h, q)
    post(None)
    for h, q in order:
        there = product((2, 1)[h], h, q)
        outs[0, h, q].wait_recv()
        sent[2, 2 * h + q] = (there + got[0, 2 * h + q].astype(f32)).astype(bf16)
        post(outs[2, h, q])
    post(None)
    for h, q in order:
        at = pl.ds((2 * h + q) * piece, piece)
        outs[1, h, q].wait_recv()
        total[:, at] = total[:, at] + got[1, 2 * h + q].astype(f32)
    for h, q in order:
        at = pl.ds((2 * h + q) * piece, piece)
        outs[2, h, q].wait_recv()
        out[:, at] = (total[:, at] + got[2, 2 * h + q].astype(f32)).astype(bf16)
    for copy in hid_above + hid_east + hid_corner + subs + [down_side, up_side]:
        copy.wait_send()
    for copy in down_across + up_across + down_relay + up_relay + list(outs.values()):
        copy.wait_send()


COPIES = 9 + 2 + 2 * (DOWN_PARTS + UP_PARTS) + 4 + 1 + 3 + 12


def scratch(rows, width, depth, model):
    every = 4 * rows
    vmem = pltpu.VMEM
    return [
        vmem((every, width), bf16),
        vmem((4, 8, rows), jnp.int32),
        vmem((4, width, depth), bf16),
        vmem((4 * depth, width), bf16),
        vmem((every, model), bf16),
        vmem((every, model), bf16),
        vmem((every, width), bf16),
        vmem((every, 4 * depth), bf16),
        vmem((every, 4 * depth), bf16),
        vmem((every, 128), f32),
        vmem((128, every), f32),
        vmem((8, every), f32),
        vmem((8, every), f32),
        vmem((8, every), f32),
        vmem((3, 8, every), f32),
        vmem((3, 4, rows, width // 4), bf16),
        vmem((3, 4, rows, width // 4), bf16),
        vmem((rows, width), f32),
        vmem((DEPTH, width, QUERY_TILE), bf16),
        vmem((DEPTH, KEY_TILE, model), bf16),
        pltpu.SemaphoreType.DMA((COPIES,)),
        pltpu.SemaphoreType.DMA((COPIES,)),
        pltpu.SemaphoreType.DMA((2 * model // QUERY_TILE,)),
        pltpu.SemaphoreType.DMA((2 * model // QUERY_TILE,)),
        pltpu.SemaphoreType.DMA((4,)),
        pltpu.SemaphoreType.DMA((DEPTH,)),
        pltpu.SemaphoreType.DMA((DEPTH,)),
    ]


def sizes_of(hidden, down_weight, query_weight):
    return hidden.shape + (down_weight.shape[2], query_weight.shape[1])


def fits(hidden, subsets, down_weight, up_weight, query_weight, key_weight):
    if lax.axis_size("adapter") != 16 or lax.axis_size("mp") != 2 or subsets.shape[1] != 8:
        return False
    rows, width, depth, model = sizes = sizes_of(hidden, down_weight, query_weight)
    if rows % 64 or depth % 128 or width % 512 or width % KEY_TILE or model % QUERY_TILE:
        return False
    buffers = [s for s in scratch(*sizes) if hasattr(s, "shape")]
    held = sum(int(np.prod(s.shape)) * jnp.dtype(s.dtype).itemsize for s in buffers[:20])
    return held + 2 * rows * width < VMEM_BYTES


def in_one_kernel(hidden, subsets, down_weight, up_weight, query_weight, key_weight):
    rows, width, depth, model = sizes_of(hidden, down_weight, query_weight)
    any_space = pl.BlockSpec(memory_space=pl.ANY)
    in_vmem = pl.BlockSpec(memory_space=pltpu.VMEM)
    return pl.pallas_call(
        functools.partial(kernel, (1, 4, 2, 8)),
        out_shape=jax.ShapeDtypeStruct((rows, width), bf16),
        in_specs=[any_space] * 6,
        out_specs=in_vmem,
        scratch_shapes=scratch(rows, width, depth, model),
        compiler_params=pltpu.CompilerParams(
            collective_id=0, has_side_effects=True, vmem_limit_bytes=VMEM_BYTES
        ),
    )(hidden, subsets.T, down_weight[0], up_weight[0], query_weight, key_weight)


def spread_out(hidden, subsets, down_weight, up_weight, query_weight, key_weight):
    n = lax.axis_size("adapter")
    rows, width = hidden.shape
    bottleneck = down_weight.shape[2]
    model_width = query_weight.shape[1]
    half = width // 2
    me = lax.axis_index("adapter")

    bits = [1 << b for b in range(n.bit_length() - 1)]
    east, above = bits[0], bits[2]
    corner = east ^ above
    class_bits = [b for b in bits if b not in (east, above)][::-1]
    blocks = [0, east, above, corner]

    def swapped(array, bit):
        return lax.ppermute(array, "adapter", [(i, i ^ bit) for i in range(n)])

    hid = {0: hidden}
    hid[above] = swapped(hidden, above)
    hid[east] = swapped(hidden, east)
    hid[corner] = swapped(hid[above], east)
    sub = {0: subsets}
    for b in blocks[1:]:
        sub[b] = swapped(subsets, b)
    subset_all = jnp.concatenate([sub[b] for b in blocks], axis=0)

    def spread(held):
        held = {0: held}
        for bit in class_bits:
            held.update({m ^ bit: swapped(block, bit) for m, block in list(held.items())})
        return held

    down = spread(down_weight[0])
    up = [spread(up_weight[0][:, :half]), spread(up_weight[0][:, half:])]
    names = list(down)

    def probe_of(h):
        query_part = jnp.dot(h, query_weight, preferred_element_type=f32)
        query = both_cores(query_part.astype(bf16))
        return lax.dot_general(
            query, key_weight, (((1,), (1,)), ((), ())), preferred_element_type=f32
        ).astype(bf16)

    probe_own = probe_of(hid[0])
    probe_next = probe_of(jnp.concatenate([hid[east], hid[above]], axis=0))
    probe_last = probe_of(hid[corner])
    hid_all = jnp.concatenate([hid[b] for b in blocks], axis=0)
    probe_all = jnp.concatenate([probe_own, probe_next, probe_last], axis=0)
    own_term = jnp.sum(hid_all.astype(f32) * probe_all.astype(f32), axis=1)

    wide, partial = {}, []
    for m in names:
        part = jnp.dot(hid_all, down[m], preferred_element_type=f32).astype(bf16)
        wide[m] = jnp.maximum(both_cores(part), 0)
    for m in names:
        reach = 0.0
        for h in range(2):
            reach = reach + lax.dot_general(
                probe_all[:, h * half : (h + 1) * half],
                up[h][m],
                (((1,), (1,)), ((), ())),
                preferred_element_type=f32,
            )
        partial.append(jnp.sum(wide[m].astype(f32) * reach, axis=1) + own_term)
    logits = both_cores(jnp.stack(partial)) * model_width ** (-0.5)

    labels = jnp.stack([me ^ m for m in names]).astype(jnp.int32)
    named = jnp.any(subset_all[None, :, :] == labels[:, None, None], axis=2)
    masked = jnp.where(named, logits, -jnp.inf)
    everyone = [masked]
    for s in blocks[1:]:
        theirs = swapped(masked, s)
        order = [blocks.index(b ^ s) for b in blocks]
        everyone.append(
            jnp.concatenate([theirs[:, o * rows : (o + 1) * rows] for o in order], axis=1)
        )
    share = jax.nn.softmax(jnp.concatenate(everyone, axis=0), axis=0)[: len(names)]
    weighted = jnp.concatenate(
        [(wide[m].astype(f32) * share[i][:, None]).astype(bf16) for i, m in enumerate(names)],
        axis=1,
    )
    tile = [jnp.concatenate([up[h][m] for m in names], axis=0) for h in range(2)]

    def output(b, h):
        i = blocks.index(b)
        return jnp.dot(weighted[i * rows : (i + 1) * rows], tile[h], preferred_element_type=f32)

    joined = []
    for h, (first, then) in enumerate([(east, above), (above, east)]):
        far = swapped(output(corner, h).astype(bf16), first)
        near = swapped(output(first, h).astype(bf16), first)
        passed = swapped((output(then, h) + far.astype(f32)).astype(bf16), then)
        base = hidden[:, h * half : (h + 1) * half].astype(f32)
        joined.append(
            (base + output(0, h) + near.astype(f32) + passed.astype(f32)).astype(bf16)
        )
    return jnp.concatenate(joined, axis=1)


def per_device(*arrays):
    form = spread_out
    if fits(*arrays):
        form = in_one_kernel
    return form(*arrays)


def solution(mesh):
    return jax.shard_map(
        per_device,
        mesh=mesh,
        in_specs=(
            P("adapter", "mp"),
            P("adapter", None),
            P("adapter", "mp", None),
            P("adapter", None, "mp"),
            P("mp", None),
            P("mp", None),
        ),
        out_specs=P("adapter", "mp"),
        check_vma=False,
    )
```

```python
import functools

import jax
import jax.numpy as jnp
import numpy as np
from jax import lax
from jax.experimental import pallas as pl
from jax.experimental.pallas import tpu as pltpu
from jax.sharding import PartitionSpec as P


f32, bf16 = jnp.float32, jnp.bfloat16


def both_cores(part):
    size = lax.axis_size("mp")
    total = part
    for shift in range(1, size):
        total = total + lax.ppermute(part, "mp", [(i, (i + shift) % size) for i in range(size)])
    return total


MESH = pl.DeviceIdType.MESH
NEVER = -1e30
VMEM_BYTES = 67_000_000
QUERY_TILE, KEY_TILE, DEPTH = 512, 256, 5
DOWN_PARTS, UP_PARTS = 2, 8
NT = (((1,), (1,)), ((), ()))


def dot(a, b):
    return jnp.dot(a, b, preferred_element_type=f32)


def dot_nt(a, b):
    return lax.dot_general(a, b, NT, preferred_element_type=f32)


def kernel(
    bits, hid_in, sub_in, down_in, up_in, query_in, key_in, out,
    hid, sub, down, up, query, query_got, probe, wide, wide_got, level, turned,
    mine, mine_got, masked, theirs, sent, got, total, query_tile, key_tile,
    send, recv, query_send, query_recv, local, query_sem, key_sem,
):
    east, above, side, across = bits
    rows, width = hid_in.shape
    model = query_in.shape[1]
    depth = down_in.shape[1]
    everyone = 4 * rows
    me, core = lax.axis_index("adapter"), lax.axis_index("mp")

    def flip(index, bit):
        return index + bit * (1 - 2 * ((index // bit) % 2))

    to_east, to_above = (flip(me, east), core), (flip(me, above), core)
    to_corner = (flip(flip(me, east), above), core)
    to_side, to_across, to_core = (flip(me, side), core), (flip(me, across), core), (me, 1 - core)

    count = [0]

    def remote(src, dst, where):
        i = count[0]
        count[0] += 1
        return pltpu.make_async_remote_copy(
            src_ref=src, dst_ref=dst, send_sem=send.at[i], recv_sem=recv.at[i],
            device_id=where, device_id_type=MESH,
        )

    def block(ref, b, start=0, size=rows):
        return ref.at[pl.ds(b * rows + start, size), :]

    half = rows // 2
    hid_above = [remote(hid_in.at[pl.ds(h * half, half), :], block(hid, 2, h * half, half), to_above) for h in (0, 1)]
    hid_east = [remote(hid_in.at[pl.ds(h * half, half), :], block(hid, 1, h * half, half), to_east) for h in (0, 1)]
    hid_corner = [
        remote(block(hid, 2, 0, half), block(hid, 3, 0, half), to_east),
        remote(block(hid, 2, half, half), block(hid, 3, half, half), to_east),
    ]
    subs = [remote(sub_in, sub.at[k], w) for k, w in ((1, to_east), (2, to_above), (3, to_corner))]

    def down_cut(ref, c):
        size = width // DOWN_PARTS
        return ref.at[pl.ds(c * size, size), :]

    def up_cut(ref, m, c):
        size = width // UP_PARTS
        return ref.at[pl.ds(m * depth, depth), pl.ds(c * size, size)]

    down_side = remote(down_in, down.at[1], to_side)
    up_side = remote(up_in, up.at[pl.ds(depth, depth), :], to_side)
    down_across = [remote(down_cut(down_in, c), down_cut(down.at[2], c), to_across) for c in range(DOWN_PARTS)]
    up_across = [remote(up_cut(up_in, 0, c), up_cut(up, 2, c), to_across) for c in range(UP_PARTS)]
    down_relay = [remote(down_cut(down.at[2], c), down_cut(down.at[3], c), to_side) for c in range(DOWN_PARTS)]
    up_relay = [remote(up_cut(up, 2, c), up_cut(up, 3, c), to_side) for c in range(UP_PARTS)]
    wides = [
        remote(wide.at[:, pl.ds(m * depth, depth)], wide_got.at[:, pl.ds(m * depth, depth)], to_core)
        for m in range(4)
    ]
    mines = remote(mine, mine_got, to_core)
    tells = [remote(masked, theirs.at[k - 1], w) for k, w in ((1, to_east), (2, to_above), (3, to_corner))]
    piece = width // 4
    hops = [(to_east, to_above), (to_above, to_east)]
    outs = {
        (kind, h, q): remote(sent.at[kind, 2 * h + q], got.at[kind, 2 * h + q], hops[h][0 if kind < 2 else 1])
        for kind in range(3) for h in range(2) for q in range(2)
    }

    own_hid = pltpu.make_async_copy(hid_in, block(hid, 0), local.at[0])
    own_down = pltpu.make_async_copy(down_in, down.at[0], local.at[1])
    own_up = pltpu.make_async_copy(up_in, up.at[pl.ds(0, depth), :], local.at[2])
    own_sub = pltpu.make_async_copy(sub_in, sub.at[0], local.at[3])

    query_tiles, key_tiles = model // QUERY_TILE, width // KEY_TILE

    def query_fetch(j):
        s = lax.rem(j, DEPTH)
        return pltpu.make_async_copy(
            query_in.at[:, pl.ds(j * QUERY_TILE, QUERY_TILE)], query_tile.at[s], query_sem.at[s])

    def key_fetch(j):
        s = lax.rem(j, DEPTH)
        return pltpu.make_async_copy(
            key_in.at[pl.ds(j * KEY_TILE, KEY_TILE), :], key_tile.at[s], key_sem.at[s])

    def ahead(fetch):
        for j in range(DEPTH - 1):
            fetch(jnp.int32(j)).start()

    def follow(fetch, j, tiles):
        @pl.when(j + (DEPTH - 1) < tiles)
        def _():
            fetch(j + (DEPTH - 1)).start()

        fetch(j).wait()

    def query_send_tile(turn, j):
        at = (slice(None), pl.ds(j * QUERY_TILE, QUERY_TILE))
        i = turn * query_tiles + j
        return pltpu.make_async_remote_copy(
            src_ref=query.at[at], dst_ref=query_got.at[(turn % 2,) + at],
            send_sem=query_send.at[i], recv_sem=query_recv.at[i],
            device_id=to_core, device_id_type=MESH,
        )

    def query_part(turn):
        def step(j, _):
            follow(query_fetch, j, query_tiles)
            tile = dot(hid[pl.ds(turn * rows, rows), :], query_tile[lax.rem(j, DEPTH)])
            query[:, pl.ds(pl.multiple_of(j * QUERY_TILE, QUERY_TILE), QUERY_TILE)] = tile.astype(bf16)

            @pl.when(j > 0)
            def _():
                query_send_tile(turn, j - 1).start()

            return 0

        lax.fori_loop(0, query_tiles, step, 0)
        query_send_tile(turn, query_tiles - 1).start()
        if turn < 3:
            ahead(query_fetch)

    def query_sum(turn):
        def step(j, _):
            query_send_tile(turn, j).wait()
            at = (slice(None), pl.ds(pl.multiple_of(j * QUERY_TILE, QUERY_TILE), QUERY_TILE))
            query[at] = query[at] + query_got[(turn % 2,) + at]
            return 0

        lax.fori_loop(0, query_tiles, step, 0)

    def probe_part(turn):
        def step(j, _):
            follow(key_fetch, j, key_tiles)
            tile = dot_nt(query[...], key_tile[lax.rem(j, DEPTH)])
            at = pl.ds(pl.multiple_of(j * KEY_TILE, KEY_TILE), KEY_TILE)
            probe[pl.ds(turn * rows, rows), at] = tile.astype(bf16)
            return 0

        lax.fori_loop(0, key_tiles, step, 0)
        if turn < 3:
            ahead(key_fetch)

    def bottle(m):
        def step(c, _):
            at = pl.ds(pl.multiple_of(c * rows, rows), rows)
            wide[at, pl.ds(m * depth, depth)] = dot(hid[at, :], down[m]).astype(bf16)
            return 0

        lax.fori_loop(0, 4, step, 0)

    def own_term():
        def step(c, _):
            at = pl.ds(pl.multiple_of(c * rows // 4, rows // 4), rows // 4)
            term = jnp.sum(hid[at, :].astype(f32) * probe[at, :].astype(f32), axis=1, keepdims=True)
            level[at, :] = jnp.broadcast_to(term, (rows // 4, level.shape[1]))
            return 0

        lax.fori_loop(0, 16, step, 0)

    def reach(m, early=0):
        columns, rest = pl.ds(m * depth, depth), pl.ds(early, width - early)

        def step(c, _):
            at = pl.ds(pl.multiple_of(c * rows, rows), rows)
            there = dot_nt(probe[at, rest], up[columns, rest])
            if early:
                there = there + total[:, pl.ds(pl.multiple_of(c * depth, depth), depth)]
            kept = jnp.maximum(wide[at, columns] + wide_got[at, columns], 0)
            wide[at, columns] = kept
            term = jnp.sum(kept.astype(f32) * there, axis=1, keepdims=True)
            lane = lax.broadcasted_iota(jnp.int32, (rows, level.shape[1]), 1)
            level[at, :] = level[at, :] + jnp.where(lane == m, term, 0.0)
            return 0

        lax.fori_loop(0, 4, step, 0)

    def reach_early(m, early):
        def step(c, _):
            at = pl.ds(pl.multiple_of(c * rows, rows), rows)
            there = dot_nt(probe[at, pl.ds(0, early)], up[pl.ds(m * depth, depth), pl.ds(0, early)])
            total[:, pl.ds(pl.multiple_of(c * depth, depth), depth)] = there
            return 0

        lax.fori_loop(0, 4, step, 0)

    barrier = pltpu.get_barrier_semaphore()
    partners = (to_east, to_above, to_corner, to_side, to_across, to_core)
    for where in partners:
        pl.semaphore_signal(barrier, inc=1, device_id=where, device_id_type=MESH)
    pl.semaphore_wait(barrier, len(partners))

    hid_above[0].start()
    hid_east[0].start()
    own_hid.start()
    ahead(query_fetch)
    hid_above[1].start()
    hid_east[1].start()
    for copy in subs + down_across + [down_side, up_side, own_down, own_up, own_sub]:
        copy.start()
    ahead(key_fetch)

    def relay(copies, relays, low, high):
        for c in range(low, high):
            copies[c].wait_recv()
            relays[c].start()

    outer = (me // above) % 2 == (me // across) % 2
    inner = jnp.logical_not(outer)
    passed = {"down": [0, 0], "up": [0, 0]}

    def forward(kind, at_ends, between):
        copies, relays = (down_across, down_relay) if kind == "down" else (up_across, up_relay)
        for k, (place, upto) in enumerate(((outer, at_ends), (inner, between))):
            low = passed[kind][k]
            passed[kind][k] = upto
            if upto > low:

                @pl.when(place)
                def _(low=low, upto=upto):
                    relay(copies, relays, low, upto)

    own_hid.wait()
    query_part(0)
    query_sum(0)
    probe_part(0)
    for h in (0, 1):
        hid_east[h].wait_recv()
    query_part(1)
    query_sum(1)

    @pl.when(inner)
    def _():
        for h in (0, 1):
            hid_above[h].wait_recv()
            hid_corner[h].start()

    probe_part(1)
    for copy in up_across:
        copy.start()

    @pl.when(outer)
    def _():
        for h in (0, 1):
            hid_above[h].wait_recv()
            hid_corner[h].start()

    forward("down", 2, 0)

    query_part(2)
    query_sum(2)
    forward("down", 2, 2)
    probe_part(2)
    for h in (0, 1):
        hid_corner[h].wait_recv()
    query_part(3)
    forward("up", 0, 1)
    query_sum(3)
    probe_part(3)
    forward("up", 2, 3)
    own_down.wait()
    bottle(0)
    wides[0].start()
    down_side.wait_recv()
    bottle(1)
    forward("up", 3, 5)
    wides[1].start()
    bottle(2)
    wides[2].start()
    forward("up", 4, 6)
    own_term()
    forward("up", 5, 6)
    own_up.wait()
    wides[0].wait()
    reach(0)
    forward("up", 5, 7)
    up_side.wait_recv()
    wides[1].wait()
    reach(1)
    forward("up", 6, 8)
    for c in range(DOWN_PARTS):
        down_relay[c].wait_recv()
    bottle(3)
    wides[3].start()
    forward("up", 8, 8)
    wides[2].wait()
    reach(2)
    wides[3].wait()
    early = UP_PARTS * 3 // 4
    for c in range(early):
        up_relay[c].wait_recv()
    reach_early(3, early * (width // UP_PARTS))
    for c in range(early, UP_PARTS):
        up_relay[c].wait_recv()
    reach(3, early * (width // UP_PARTS))

    mine[...] = jnp.transpose(level[...])[:8]
    for copy in subs:
        copy.wait_recv()
    own_sub.wait()
    turned[...] = jnp.zeros_like(turned)
    line = lax.broadcasted_iota(jnp.int32, (8, rows), 0)
    labels = [me, flip(me, side), flip(me, across), flip(flip(me, side), across)]
    named = []
    for b in range(4):
        marks = jnp.zeros((8, rows), f32)
        for m in range(4):
            hit = jnp.max((sub[b] == labels[m]).astype(f32), axis=0, keepdims=True)
            marks = jnp.where(line == m, hit, marks)
        named.append(marks)
    mines.start()
    mines.wait()
    for b in range(4):
        at = pl.ds(b * rows, rows)
        logit = (mine[:, at] + mine_got[:, at]) * model ** (-0.5)
        masked[:, at] = jnp.where(named[b] > 0, logit, NEVER)
    for copy in tells:
        copy.start()
    for copy in tells:
        copy.wait()
    for b in range(4):
        at = pl.ds(b * rows, rows)
        own = masked[:, at]
        others = [theirs[k - 1][:, (b ^ k) * rows : ((b ^ k) + 1) * rows] for k in (1, 2, 3)]
        peak = own
        for other in others:
            peak = jnp.maximum(peak, other)
        peak = jnp.max(peak, axis=0, keepdims=True)
        mass = jnp.exp(own - peak)
        whole = mass
        for other in others:
            whole = whole + jnp.exp(other - peak)
        turned[0:8, at] = mass / jnp.sum(whole, axis=0, keepdims=True)
    level[...] = jnp.transpose(turned[...])

    def weigh(b):
        at = pl.ds(b * rows, rows)
        for m in range(4):
            columns = pl.ds(m * depth, depth)
            wide[at, columns] = (wide[at, columns].astype(f32) * level[at, m : m + 1]).astype(bf16)

    def product(b, h, q):
        return dot(wide[pl.ds(b * rows, rows), :], up[:, pl.ds((2 * h + q) * piece, piece)])

    pending = []

    def post(copy):
        if pending:
            pending.pop().start()
        if copy is not None:
            pending.append(copy)

    order = [(h, q) for q in range(2) for h in range(2)]
    weigh(3)
    for h, q in order:
        sent[0, 2 * h + q] = product(3, h, q).astype(bf16)
        post(outs[0, h, q])
    weigh(1)
    weigh(2)
    for h, q in order:
        sent[1, 2 * h + q] = product((1, 2)[h], h, q).astype(bf16)
        post(outs[1, h, q])
    weigh(0)
    for h, q in order:
        at = pl.ds((2 * h + q) * piece, piece)
        total[:, at] = hid[pl.ds(0, rows), at].astype(f32) + product(0, h, q)
    post(None)
    for h, q in order:
        there = product((2, 1)[h], h, q)
        outs[0, h, q].wait_recv()
        sent[2, 2 * h + q] = (there + got[0, 2 * h + q].astype(f32)).astype(bf16)
        post(outs[2, h, q])
    post(None)
    for h, q in order:
        at = pl.ds((2 * h + q) * piece, piece)
        outs[1, h, q].wait_recv()
        total[:, at] = total[:, at] + got[1, 2 * h + q].astype(f32)
    for h, q in order:
        at = pl.ds((2 * h + q) * piece, piece)
        outs[2, h, q].wait_recv()
        out[:, at] = (total[:, at] + got[2, 2 * h + q].astype(f32)).astype(bf16)
    for copy in hid_above + hid_east + hid_corner + subs + [down_side, up_side]:
        copy.wait_send()
    for copy in down_across + up_across + down_relay + up_relay + list(outs.values()):
        copy.wait_send()


COPIES = 9 + 2 + 2 * (DOWN_PARTS + UP_PARTS) + 4 + 1 + 3 + 12


def scratch(rows, width, depth, model):
    every = 4 * rows
    vmem = pltpu.VMEM
    return [
        vmem((every, width), bf16),
        vmem((4, 8, rows), jnp.int32),
        vmem((4, width, depth), bf16),
        vmem((4 * depth, width), bf16),
        vmem((rows, model), bf16),
        vmem((2, rows, model), bf16),
        vmem((every, width), bf16),
        vmem((every, 4 * depth), bf16),
        vmem((every, 4 * depth), bf16),
        vmem((every, 128), f32),
        vmem((128, every), f32),
        vmem((8, every), f32),
        vmem((8, every), f32),
        vmem((8, every), f32),
        vmem((3, 8, every), f32),
        vmem((3, 4, rows, width // 4), bf16),
        vmem((3, 4, rows, width // 4), bf16),
        vmem((rows, width), f32),
        vmem((DEPTH, width, QUERY_TILE), bf16),
        vmem((DEPTH, KEY_TILE, model), bf16),
        pltpu.SemaphoreType.DMA((COPIES,)),
        pltpu.SemaphoreType.DMA((COPIES,)),
        pltpu.SemaphoreType.DMA((4 * model // QUERY_TILE,)),
        pltpu.SemaphoreType.DMA((4 * model // QUERY_TILE,)),
        pltpu.SemaphoreType.DMA((4,)),
        pltpu.SemaphoreType.DMA((DEPTH,)),
        pltpu.SemaphoreType.DMA((DEPTH,)),
    ]


def sizes_of(hidden, down_weight, query_weight):
    return hidden.shape + (down_weight.shape[2], query_weight.shape[1])


def fits(hidden, subsets, down_weight, up_weight, query_weight, key_weight):
    if lax.axis_size("adapter") != 16 or lax.axis_size("mp") != 2 or subsets.shape[1] != 8:
        return False
    rows, width, depth, model = sizes = sizes_of(hidden, down_weight, query_weight)
    if rows % 64 or depth % 128 or width % 512 or width % KEY_TILE or model % QUERY_TILE:
        return False
    buffers = [s for s in scratch(*sizes) if hasattr(s, "shape")]
    held = sum(int(np.prod(s.shape)) * jnp.dtype(s.dtype).itemsize for s in buffers[:20])
    return held + 2 * rows * width < VMEM_BYTES


def in_one_kernel(hidden, subsets, down_weight, up_weight, query_weight, key_weight):
    rows, width, depth, model = sizes_of(hidden, down_weight, query_weight)
    any_space = pl.BlockSpec(memory_space=pl.ANY)
    in_vmem = pl.BlockSpec(memory_space=pltpu.VMEM)
    return pl.pallas_call(
        functools.partial(kernel, (1, 4, 2, 8)),
        out_shape=jax.ShapeDtypeStruct((rows, width), bf16),
        in_specs=[any_space] * 6,
        out_specs=in_vmem,
        scratch_shapes=scratch(rows, width, depth, model),
        compiler_params=pltpu.CompilerParams(
            collective_id=0, has_side_effects=True, vmem_limit_bytes=VMEM_BYTES
        ),
    )(hidden, subsets.T, down_weight[0], up_weight[0], query_weight, key_weight)


def spread_out(hidden, subsets, down_weight, up_weight, query_weight, key_weight):
    n = lax.axis_size("adapter")
    rows, width = hidden.shape
    bottleneck = down_weight.shape[2]
    model_width = query_weight.shape[1]
    half = width // 2
    me = lax.axis_index("adapter")

    bits = [1 << b for b in range(n.bit_length() - 1)]
    east, above = bits[0], bits[2]
    corner = east ^ above
    class_bits = [b for b in bits if b not in (east, above)][::-1]
    blocks = [0, east, above, corner]

    def swapped(array, bit):
        return lax.ppermute(array, "adapter", [(i, i ^ bit) for i in range(n)])

    hid = {0: hidden}
    hid[above] = swapped(hidden, above)
    hid[east] = swapped(hidden, east)
    hid[corner] = swapped(hid[above], east)
    sub = {0: subsets}
    for b in blocks[1:]:
        sub[b] = swapped(subsets, b)
    subset_all = jnp.concatenate([sub[b] for b in blocks], axis=0)

    def spread(held):
        held = {0: held}
        for bit in class_bits:
            held.update({m ^ bit: swapped(block, bit) for m, block in list(held.items())})
        return held

    down = spread(down_weight[0])
    up = [spread(up_weight[0][:, :half]), spread(up_weight[0][:, half:])]
    names = list(down)

    def probe_of(h):
        query_part = jnp.dot(h, query_weight, preferred_element_type=f32)
        query = both_cores(query_part.astype(bf16))
        return lax.dot_general(
            query, key_weight, (((1,), (1,)), ((), ())), preferred_element_type=f32
        ).astype(bf16)

    probe_own = probe_of(hid[0])
    probe_next = probe_of(jnp.concatenate([hid[east], hid[above]], axis=0))
    probe_last = probe_of(hid[corner])
    hid_all = jnp.concatenate([hid[b] for b in blocks], axis=0)
    probe_all = jnp.concatenate([probe_own, probe_next, probe_last], axis=0)
    own_term = jnp.sum(hid_all.astype(f32) * probe_all.astype(f32), axis=1)

    wide, partial = {}, []
    for m in names:
        part = jnp.dot(hid_all, down[m], preferred_element_type=f32).astype(bf16)
        wide[m] = jnp.maximum(both_cores(part), 0)
    for m in names:
        reach = 0.0
        for h in range(2):
            reach = reach + lax.dot_general(
                probe_all[:, h * half : (h + 1) * half],
                up[h][m],
                (((1,), (1,)), ((), ())),
                preferred_element_type=f32,
            )
        partial.append(jnp.sum(wide[m].astype(f32) * reach, axis=1) + own_term)
    logits = both_cores(jnp.stack(partial)) * model_width ** (-0.5)

    labels = jnp.stack([me ^ m for m in names]).astype(jnp.int32)
    named = jnp.any(subset_all[None, :, :] == labels[:, None, None], axis=2)
    masked = jnp.where(named, logits, -jnp.inf)
    everyone = [masked]
    for s in blocks[1:]:
        theirs = swapped(masked, s)
        order = [blocks.index(b ^ s) for b in blocks]
        everyone.append(
            jnp.concatenate([theirs[:, o * rows : (o + 1) * rows] for o in order], axis=1)
        )
    share = jax.nn.softmax(jnp.concatenate(everyone, axis=0), axis=0)[: len(names)]
    weighted = jnp.concatenate(
        [(wide[m].astype(f32) * share[i][:, None]).astype(bf16) for i, m in enumerate(names)],
        axis=1,
    )
    tile = [jnp.concatenate([up[h][m] for m in names], axis=0) for h in range(2)]

    def output(b, h):
        i = blocks.index(b)
        return jnp.dot(weighted[i * rows : (i + 1) * rows], tile[h], preferred_element_type=f32)

    joined = []
    for h, (first, then) in enumerate([(east, above), (above, east)]):
        far = swapped(output(corner, h).astype(bf16), first)
        near = swapped(output(first, h).astype(bf16), first)
        passed = swapped((output(then, h) + far.astype(f32)).astype(bf16), then)
        base = hidden[:, h * half : (h + 1) * half].astype(f32)
        joined.append(
            (base + output(0, h) + near.astype(f32) + passed.astype(f32)).astype(bf16)
        )
    return jnp.concatenate(joined, axis=1)


def per_device(*arrays):
    form = spread_out
    if fits(*arrays):
        form = in_one_kernel
    return form(*arrays)


def solution(mesh):
    return jax.shard_map(
        per_device,
        mesh=mesh,
        in_specs=(
            P("adapter", "mp"),
            P("adapter", None),
            P("adapter", "mp", None),
            P("adapter", None, "mp"),
            P("mp", None),
            P("mp", None),
        ),
        out_specs=P("adapter", "mp"),
        check_vma=False,
    )
```

```python
import functools

import jax
import jax.numpy as jnp
import numpy as np
from jax import lax
from jax.experimental import pallas as pl
from jax.experimental.pallas import tpu as pltpu
from jax.sharding import PartitionSpec as P


f32, bf16 = jnp.float32, jnp.bfloat16


def both_cores(part):
    size = lax.axis_size("mp")
    total = part
    for shift in range(1, size):
        total = total + lax.ppermute(part, "mp", [(i, (i + shift) % size) for i in range(size)])
    return total


MESH = pl.DeviceIdType.MESH
NEVER = -1e30
VMEM_BYTES = 67_000_000
QUERY_TILE, KEY_TILE, DEPTH = 512, 256, 5
DOWN_PARTS, UP_PARTS = 2, 16
NT = (((1,), (1,)), ((), ()))


def dot(a, b):
    return jnp.dot(a, b, preferred_element_type=f32)


def dot_nt(a, b):
    return lax.dot_general(a, b, NT, preferred_element_type=f32)


def kernel(
    bits, hid_in, sub_in, down_in, up_in, query_in, key_in, out,
    hid, sub, down, up, query, query_got, probe, wide, wide_got, level, turned,
    mine, mine_got, masked, theirs, sent, got, total, query_tile, key_tile,
    send, recv, query_send, query_recv, local, query_sem, key_sem,
):
    east, above, side, across = bits
    rows, width = hid_in.shape
    model = query_in.shape[1]
    depth = down_in.shape[1]
    everyone = 4 * rows
    me, core = lax.axis_index("adapter"), lax.axis_index("mp")

    def flip(index, bit):
        return index + bit * (1 - 2 * ((index // bit) % 2))

    to_east, to_above = (flip(me, east), core), (flip(me, above), core)
    to_corner = (flip(flip(me, east), above), core)
    to_side, to_across, to_core = (flip(me, side), core), (flip(me, across), core), (me, 1 - core)

    count = [0]

    def remote(src, dst, where):
        i = count[0]
        count[0] += 1
        return pltpu.make_async_remote_copy(
            src_ref=src, dst_ref=dst, send_sem=send.at[i], recv_sem=recv.at[i],
            device_id=where, device_id_type=MESH,
        )

    def block(ref, b, start=0, size=rows):
        return ref.at[pl.ds(b * rows + start, size), :]

    half = rows // 2
    hid_above = [remote(hid_in.at[pl.ds(h * half, half), :], block(hid, 2, h * half, half), to_above) for h in (0, 1)]
    hid_east = [remote(hid_in.at[pl.ds(h * half, half), :], block(hid, 1, h * half, half), to_east) for h in (0, 1)]
    hid_corner = [
        remote(block(hid, 2, 0, half), block(hid, 3, 0, half), to_east),
        remote(block(hid, 2, half, half), block(hid, 3, half, half), to_east),
    ]
    subs = [remote(sub_in, sub.at[k], w) for k, w in ((1, to_east), (2, to_above), (3, to_corner))]

    def down_cut(ref, c):
        size = width // DOWN_PARTS
        return ref.at[pl.ds(c * size, size), :]

    def up_cut(ref, m, c):
        size = width // UP_PARTS
        return ref.at[pl.ds(m * depth, depth), pl.ds(c * size, size)]

    down_side = remote(down_in, down.at[1], to_side)
    up_side = remote(up_in, up.at[pl.ds(depth, depth), :], to_side)
    down_across = [remote(down_cut(down_in, c), down_cut(down.at[2], c), to_across) for c in range(DOWN_PARTS)]
    up_across = [remote(up_cut(up_in, 0, c), up_cut(up, 2, c), to_across) for c in range(UP_PARTS)]
    down_relay = [remote(down_cut(down.at[2], c), down_cut(down.at[3], c), to_side) for c in range(DOWN_PARTS)]
    up_relay = [remote(up_cut(up, 2, c), up_cut(up, 3, c), to_side) for c in range(UP_PARTS)]
    wides = [
        remote(wide.at[:, pl.ds(m * depth, depth)], wide_got.at[:, pl.ds(m * depth, depth)], to_core)
        for m in range(4)
    ]
    mines = remote(mine, mine_got, to_core)
    tells = [remote(masked, theirs.at[k - 1], w) for k, w in ((1, to_east), (2, to_above), (3, to_corner))]
    piece = width // 4
    hops = [(to_east, to_above), (to_above, to_east)]
    outs = {
        (kind, h, q): remote(sent.at[kind, 2 * h + q], got.at[kind, 2 * h + q], hops[h][0 if kind < 2 else 1])
        for kind in range(3) for h in range(2) for q in range(2)
    }

    own_hid = pltpu.make_async_copy(hid_in, block(hid, 0), local.at[0])
    own_down = pltpu.make_async_copy(down_in, down.at[0], local.at[1])
    own_up = pltpu.make_async_copy(up_in, up.at[pl.ds(0, depth), :], local.at[2])
    own_sub = pltpu.make_async_copy(sub_in, sub.at[0], local.at[3])

    query_tiles, key_tiles = model // QUERY_TILE, width // KEY_TILE

    def query_fetch(j):
        s = lax.rem(j, DEPTH)
        return pltpu.make_async_copy(
            query_in.at[:, pl.ds(j * QUERY_TILE, QUERY_TILE)], query_tile.at[s], query_sem.at[s])

    def key_fetch(j):
        s = lax.rem(j, DEPTH)
        return pltpu.make_async_copy(
            key_in.at[pl.ds(j * KEY_TILE, KEY_TILE), :], key_tile.at[s], key_sem.at[s])

    def ahead(fetch):
        for j in range(DEPTH - 1):
            fetch(jnp.int32(j)).start()

    def follow(fetch, j, tiles):
        @pl.when(j + (DEPTH - 1) < tiles)
        def _():
            fetch(j + (DEPTH - 1)).start()

        fetch(j).wait()

    def query_send_tile(turn, j):
        at = (slice(None), pl.ds(j * QUERY_TILE, QUERY_TILE))
        i = turn * query_tiles + j
        return pltpu.make_async_remote_copy(
            src_ref=query.at[at], dst_ref=query_got.at[(turn % 2,) + at],
            send_sem=query_send.at[i], recv_sem=query_recv.at[i],
            device_id=to_core, device_id_type=MESH,
        )

    def query_part(turn):
        def step(j, _):
            follow(query_fetch, j, query_tiles)
            tile = dot(hid[pl.ds(turn * rows, rows), :], query_tile[lax.rem(j, DEPTH)])
            query[:, pl.ds(pl.multiple_of(j * QUERY_TILE, QUERY_TILE), QUERY_TILE)] = tile.astype(bf16)

            @pl.when(j > 0)
            def _():
                query_send_tile(turn, j - 1).start()

            return 0

        lax.fori_loop(0, query_tiles, step, 0)
        query_send_tile(turn, query_tiles - 1).start()
        if turn < 3:
            ahead(query_fetch)

    def query_sum(turn):
        def step(j, _):
            query_send_tile(turn, j).wait()
            at = (slice(None), pl.ds(pl.multiple_of(j * QUERY_TILE, QUERY_TILE), QUERY_TILE))
            query[at] = query[at] + query_got[(turn % 2,) + at]
            return 0

        lax.fori_loop(0, query_tiles, step, 0)

    def probe_part(turn, low=0, high=key_tiles):
        def step(j, _):
            follow(key_fetch, j, key_tiles)
            tile = dot_nt(query[...], key_tile[lax.rem(j, DEPTH)])
            at = pl.ds(pl.multiple_of(j * KEY_TILE, KEY_TILE), KEY_TILE)
            probe[pl.ds(turn * rows, rows), at] = tile.astype(bf16)
            return 0

        lax.fori_loop(low, high, step, 0)
        if turn < 3:
            ahead(key_fetch)

    def bottle(m):
        def step(c, _):
            at = pl.ds(pl.multiple_of(c * rows, rows), rows)
            wide[at, pl.ds(m * depth, depth)] = dot(hid[at, :], down[m]).astype(bf16)
            return 0

        lax.fori_loop(0, 4, step, 0)

    def own_term():
        def step(c, _):
            at = pl.ds(pl.multiple_of(c * rows // 4, rows // 4), rows // 4)
            term = jnp.sum(hid[at, :].astype(f32) * probe[at, :].astype(f32), axis=1, keepdims=True)
            level[at, :] = jnp.broadcast_to(term, (rows // 4, level.shape[1]))
            return 0

        lax.fori_loop(0, 16, step, 0)

    def reach(m, early=0):
        columns, rest = pl.ds(m * depth, depth), pl.ds(early, width - early)

        def step(c, _):
            at = pl.ds(pl.multiple_of(c * rows, rows), rows)
            there = dot_nt(probe[at, rest], up[columns, rest])
            if early:
                there = there + total[:, pl.ds(pl.multiple_of(c * depth, depth), depth)]
            kept = jnp.maximum(wide[at, columns] + wide_got[at, columns], 0)
            wide[at, columns] = kept
            term = jnp.sum(kept.astype(f32) * there, axis=1, keepdims=True)
            lane = lax.broadcasted_iota(jnp.int32, (rows, level.shape[1]), 1)
            level[at, :] = level[at, :] + jnp.where(lane == m, term, 0.0)
            return 0

        lax.fori_loop(0, 4, step, 0)

    def reach_early(m, early):
        def step(c, _):
            at = pl.ds(pl.multiple_of(c * rows, rows), rows)
            there = dot_nt(probe[at, pl.ds(0, early)], up[pl.ds(m * depth, depth), pl.ds(0, early)])
            total[:, pl.ds(pl.multiple_of(c * depth, depth), depth)] = there
            return 0

        lax.fori_loop(0, 4, step, 0)

    barrier = pltpu.get_barrier_semaphore()
    partners = (to_east, to_above, to_corner, to_side, to_across, to_core)
    for where in partners:
        pl.semaphore_signal(barrier, inc=1, device_id=where, device_id_type=MESH)
    pl.semaphore_wait(barrier, len(partners))

    hid_above[0].start()
    hid_east[0].start()
    own_hid.start()
    ahead(query_fetch)
    hid_above[1].start()
    hid_east[1].start()
    for copy in subs + down_across + [down_side, up_side, own_down, own_up, own_sub]:
        copy.start()
    ahead(key_fetch)

    def relay(copies, relays, low, high):
        for c in range(low, high):
            copies[c].wait_recv()
            relays[c].start()

    outer = (me // above) % 2 == (me // across) % 2
    inner = jnp.logical_not(outer)
    passed = {"down": [0, 0], "up": [0, 0]}

    def forward(kind, at_ends, between):
        copies, relays = (down_across, down_relay) if kind == "down" else (up_across, up_relay)
        for k, (place, upto) in enumerate(((outer, at_ends), (inner, between))):
            low = passed[kind][k]
            passed[kind][k] = upto
            if upto > low:

                @pl.when(place)
                def _(low=low, upto=upto):
                    relay(copies, relays, low, upto)

    own_hid.wait()
    query_part(0)
    query_sum(0)
    probe_part(0)
    for h in (0, 1):
        hid_east[h].wait_recv()
    query_part(1)
    query_sum(1)

    @pl.when(inner)
    def _():
        for h in (0, 1):
            hid_above[h].wait_recv()
            hid_corner[h].start()

    probe_part(1)
    for copy in up_across:
        copy.start()

    @pl.when(outer)
    def _():
        for h in (0, 1):
            hid_above[h].wait_recv()
            hid_corner[h].start()

    forward("down", 2, 0)

    query_part(2)
    query_sum(2)
    forward("down", 2, 2)
    probe_part(2)
    for h in (0, 1):
        hid_corner[h].wait_recv()
    query_part(3)
    forward("up", 0, 2)
    query_sum(3)
    probe_part(3, 0, key_tiles // 2)
    forward("up", 1, 4)
    probe_part(3, key_tiles // 2, key_tiles)
    forward("up", 3, 6)
    own_down.wait()
    bottle(0)
    wides[0].start()
    forward("up", 4, 8)
    down_side.wait_recv()
    bottle(1)
    forward("up", 5, 10)
    wides[1].start()
    bottle(2)
    wides[2].start()
    forward("up", 7, 12)
    own_term()
    forward("up", 9, 13)
    own_up.wait()
    wides[0].wait()
    reach(0)
    forward("up", 10, 14)
    up_side.wait_recv()
    wides[1].wait()
    reach(1)
    forward("up", 12, 16)
    for c in range(DOWN_PARTS):
        down_relay[c].wait_recv()
    bottle(3)
    wides[3].start()
    forward("up", 16, 16)
    wides[2].wait()
    reach(2)
    wides[3].wait()
    early = UP_PARTS * 3 // 4
    for c in range(early):
        up_relay[c].wait_recv()
    reach_early(3, early * (width // UP_PARTS))
    for c in range(early, UP_PARTS):
        up_relay[c].wait_recv()
    reach(3, early * (width // UP_PARTS))

    mine[...] = jnp.transpose(level[...])[:8]
    for copy in subs:
        copy.wait_recv()
    own_sub.wait()
    turned[...] = jnp.zeros_like(turned)
    line = lax.broadcasted_iota(jnp.int32, (8, rows), 0)
    labels = [me, flip(me, side), flip(me, across), flip(flip(me, side), across)]
    named = []
    for b in range(4):
        marks = jnp.zeros((8, rows), f32)
        for m in range(4):
            hit = jnp.max((sub[b] == labels[m]).astype(f32), axis=0, keepdims=True)
            marks = jnp.where(line == m, hit, marks)
        named.append(marks)
    mines.start()
    mines.wait()
    for b in range(4):
        at = pl.ds(b * rows, rows)
        logit = (mine[:, at] + mine_got[:, at]) * model ** (-0.5)
        masked[:, at] = jnp.where(named[b] > 0, logit, NEVER)
    for copy in tells:
        copy.start()
    for copy in tells:
        copy.wait()
    for b in range(4):
        at = pl.ds(b * rows, rows)
        own = masked[:, at]
        others = [theirs[k - 1][:, (b ^ k) * rows : ((b ^ k) + 1) * rows] for k in (1, 2, 3)]
        peak = own
        for other in others:
            peak = jnp.maximum(peak, other)
        peak = jnp.max(peak, axis=0, keepdims=True)
        mass = jnp.exp(own - peak)
        whole = mass
        for other in others:
            whole = whole + jnp.exp(other - peak)
        turned[0:8, at] = mass / jnp.sum(whole, axis=0, keepdims=True)
    level[...] = jnp.transpose(turned[...])

    def weigh(b):
        at = pl.ds(b * rows, rows)
        for m in range(4):
            columns = pl.ds(m * depth, depth)
            wide[at, columns] = (wide[at, columns].astype(f32) * level[at, m : m + 1]).astype(bf16)

    def product(b, h, q):
        return dot(wide[pl.ds(b * rows, rows), :], up[:, pl.ds((2 * h + q) * piece, piece)])

    pending = []

    def post(copy):
        if pending:
            pending.pop().start()
        if copy is not None:
            pending.append(copy)

    order = [(h, q) for q in range(2) for h in range(2)]
    weigh(3)
    for h, q in order:
        sent[0, 2 * h + q] = product(3, h, q).astype(bf16)
        post(outs[0, h, q])
    weigh(1)
    weigh(2)
    for h, q in order:
        sent[1, 2 * h + q] = product((1, 2)[h], h, q).astype(bf16)
        post(outs[1, h, q])
    weigh(0)
    for h, q in order:
        at = pl.ds((2 * h + q) * piece, piece)
        total[:, at] = hid[pl.ds(0, rows), at].astype(f32) + product(0, h, q)
    post(None)
    for h, q in order:
        there = product((2, 1)[h], h, q)
        outs[0, h, q].wait_recv()
        sent[2, 2 * h + q] = (there + got[0, 2 * h + q].astype(f32)).astype(bf16)
        post(outs[2, h, q])
    post(None)
    for h, q in order:
        at = pl.ds((2 * h + q) * piece, piece)
        outs[1, h, q].wait_recv()
        total[:, at] = total[:, at] + got[1, 2 * h + q].astype(f32)
    for h, q in order:
        at = pl.ds((2 * h + q) * piece, piece)
        outs[2, h, q].wait_recv()
        out[:, at] = (total[:, at] + got[2, 2 * h + q].astype(f32)).astype(bf16)
    for copy in hid_above + hid_east + hid_corner + subs + [down_side, up_side]:
        copy.wait_send()
    for copy in down_across + up_across + down_relay + up_relay + list(outs.values()):
        copy.wait_send()


COPIES = 9 + 2 + 2 * (DOWN_PARTS + UP_PARTS) + 4 + 1 + 3 + 12


def scratch(rows, width, depth, model):
    every = 4 * rows
    vmem = pltpu.VMEM
    return [
        vmem((every, width), bf16),
        vmem((4, 8, rows), jnp.int32),
        vmem((4, width, depth), bf16),
        vmem((4 * depth, width), bf16),
        vmem((rows, model), bf16),
        vmem((2, rows, model), bf16),
        vmem((every, width), bf16),
        vmem((every, 4 * depth), bf16),
        vmem((every, 4 * depth), bf16),
        vmem((every, 128), f32),
        vmem((128, every), f32),
        vmem((8, every), f32),
        vmem((8, every), f32),
        vmem((8, every), f32),
        vmem((3, 8, every), f32),
        vmem((3, 4, rows, width // 4), bf16),
        vmem((3, 4, rows, width // 4), bf16),
        vmem((rows, width), f32),
        vmem((DEPTH, width, QUERY_TILE), bf16),
        vmem((DEPTH, KEY_TILE, model), bf16),
        pltpu.SemaphoreType.DMA((COPIES,)),
        pltpu.SemaphoreType.DMA((COPIES,)),
        pltpu.SemaphoreType.DMA((4 * model // QUERY_TILE,)),
        pltpu.SemaphoreType.DMA((4 * model // QUERY_TILE,)),
        pltpu.SemaphoreType.DMA((4,)),
        pltpu.SemaphoreType.DMA((DEPTH,)),
        pltpu.SemaphoreType.DMA((DEPTH,)),
    ]


def sizes_of(hidden, down_weight, query_weight):
    return hidden.shape + (down_weight.shape[2], query_weight.shape[1])


def fits(hidden, subsets, down_weight, up_weight, query_weight, key_weight):
    if lax.axis_size("adapter") != 16 or lax.axis_size("mp") != 2 or subsets.shape[1] != 8:
        return False
    rows, width, depth, model = sizes = sizes_of(hidden, down_weight, query_weight)
    if rows % 64 or depth % 128 or width % 512 or width % KEY_TILE or model % QUERY_TILE:
        return False
    buffers = [s for s in scratch(*sizes) if hasattr(s, "shape")]
    held = sum(int(np.prod(s.shape)) * jnp.dtype(s.dtype).itemsize for s in buffers[:20])
    return held + 2 * rows * width < VMEM_BYTES


def in_one_kernel(hidden, subsets, down_weight, up_weight, query_weight, key_weight):
    rows, width, depth, model = sizes_of(hidden, down_weight, query_weight)
    any_space = pl.BlockSpec(memory_space=pl.ANY)
    in_vmem = pl.BlockSpec(memory_space=pltpu.VMEM)
    return pl.pallas_call(
        functools.partial(kernel, (1, 4, 2, 8)),
        out_shape=jax.ShapeDtypeStruct((rows, width), bf16),
        in_specs=[any_space] * 6,
        out_specs=in_vmem,
        scratch_shapes=scratch(rows, width, depth, model),
        compiler_params=pltpu.CompilerParams(
            collective_id=0, has_side_effects=True, vmem_limit_bytes=VMEM_BYTES
        ),
    )(hidden, subsets.T, down_weight[0], up_weight[0], query_weight, key_weight)


def spread_out(hidden, subsets, down_weight, up_weight, query_weight, key_weight):
    n = lax.axis_size("adapter")
    rows, width = hidden.shape
    bottleneck = down_weight.shape[2]
    model_width = query_weight.shape[1]
    half = width // 2
    me = lax.axis_index("adapter")

    bits = [1 << b for b in range(n.bit_length() - 1)]
    east, above = bits[0], bits[2]
    corner = east ^ above
    class_bits = [b for b in bits if b not in (east, above)][::-1]
    blocks = [0, east, above, corner]

    def swapped(array, bit):
        return lax.ppermute(array, "adapter", [(i, i ^ bit) for i in range(n)])

    hid = {0: hidden}
    hid[above] = swapped(hidden, above)
    hid[east] = swapped(hidden, east)
    hid[corner] = swapped(hid[above], east)
    sub = {0: subsets}
    for b in blocks[1:]:
        sub[b] = swapped(subsets, b)
    subset_all = jnp.concatenate([sub[b] for b in blocks], axis=0)

    def spread(held):
        held = {0: held}
        for bit in class_bits:
            held.update({m ^ bit: swapped(block, bit) for m, block in list(held.items())})
        return held

    down = spread(down_weight[0])
    up = [spread(up_weight[0][:, :half]), spread(up_weight[0][:, half:])]
    names = list(down)

    def probe_of(h):
        query_part = jnp.dot(h, query_weight, preferred_element_type=f32)
        query = both_cores(query_part.astype(bf16))
        return lax.dot_general(
            query, key_weight, (((1,), (1,)), ((), ())), preferred_element_type=f32
        ).astype(bf16)

    probe_own = probe_of(hid[0])
    probe_next = probe_of(jnp.concatenate([hid[east], hid[above]], axis=0))
    probe_last = probe_of(hid[corner])
    hid_all = jnp.concatenate([hid[b] for b in blocks], axis=0)
    probe_all = jnp.concatenate([probe_own, probe_next, probe_last], axis=0)
    own_term = jnp.sum(hid_all.astype(f32) * probe_all.astype(f32), axis=1)

    wide, partial = {}, []
    for m in names:
        part = jnp.dot(hid_all, down[m], preferred_element_type=f32).astype(bf16)
        wide[m] = jnp.maximum(both_cores(part), 0)
    for m in names:
        reach = 0.0
        for h in range(2):
            reach = reach + lax.dot_general(
                probe_all[:, h * half : (h + 1) * half],
                up[h][m],
                (((1,), (1,)), ((), ())),
                preferred_element_type=f32,
            )
        partial.append(jnp.sum(wide[m].astype(f32) * reach, axis=1) + own_term)
    logits = both_cores(jnp.stack(partial)) * model_width ** (-0.5)

    labels = jnp.stack([me ^ m for m in names]).astype(jnp.int32)
    named = jnp.any(subset_all[None, :, :] == labels[:, None, None], axis=2)
    masked = jnp.where(named, logits, -jnp.inf)
    everyone = [masked]
    for s in blocks[1:]:
        theirs = swapped(masked, s)
        order = [blocks.index(b ^ s) for b in blocks]
        everyone.append(
            jnp.concatenate([theirs[:, o * rows : (o + 1) * rows] for o in order], axis=1)
        )
    share = jax.nn.softmax(jnp.concatenate(everyone, axis=0), axis=0)[: len(names)]
    weighted = jnp.concatenate(
        [(wide[m].astype(f32) * share[i][:, None]).astype(bf16) for i, m in enumerate(names)],
        axis=1,
    )
    tile = [jnp.concatenate([up[h][m] for m in names], axis=0) for h in range(2)]

    def output(b, h):
        i = blocks.index(b)
        return jnp.dot(weighted[i * rows : (i + 1) * rows], tile[h], preferred_element_type=f32)

    joined = []
    for h, (first, then) in enumerate([(east, above), (above, east)]):
        far = swapped(output(corner, h).astype(bf16), first)
        near = swapped(output(first, h).astype(bf16), first)
        passed = swapped((output(then, h) + far.astype(f32)).astype(bf16), then)
        base = hidden[:, h * half : (h + 1) * half].astype(f32)
        joined.append(
            (base + output(0, h) + near.astype(f32) + passed.astype(f32)).astype(bf16)
        )
    return jnp.concatenate(joined, axis=1)


def per_device(*arrays):
    form = spread_out
    if fits(*arrays):
        form = in_one_kernel
    return form(*arrays)


def solution(mesh):
    return jax.shard_map(
        per_device,
        mesh=mesh,
        in_specs=(
            P("adapter", "mp"),
            P("adapter", None),
            P("adapter", "mp", None),
            P("adapter", None, "mp"),
            P("mp", None),
            P("mp", None),
        ),
        out_specs=P("adapter", "mp"),
        check_vma=False,
    )
```
